32 devices in a mesh: leaf: 8 (over z, x), rows: 4 (over y, core).
Axes of the slice: x: 2, y: 2, z: 4, core: 2. Of those that a mesh axis runs over, the one named last changes fastest.
Arguments:
- right_side: float32 [8, 32768], P(None, ('leaf', 'rows')), may hold values from -6 to 6
- diagonal: float32 [32768], P(('leaf', 'rows')), may hold values from 0.5 to 4
- tree_order: int32 [32768], P(('leaf', 'rows')), may hold values from 0 to 32767, as said below
- mid_perm: int32 [8], replicated, may hold values from 0 to 7, each once
- col_factor: bfloat16 [32768, 384], P(('leaf', 'rows')), may hold values from -0.1875 to 0.1875
- mid_factor: bfloat16 [3072, 768], P('leaf', 'rows'), may hold values from -0.15625 to 0.15625
- pre_factor: bfloat16 [3072, 768], P('leaf', 'rows'), may hold values from -0.15625 to 0.15625
- row_factor: bfloat16 [48, 32768], P(None, ('leaf', 'rows')), may hold values from -0.875 to 0.875
Outputs:
- solution: float32 [8, 32768], P(None, ('leaf', 'rows'))
- residual: float32 [8, 32768], P(None, ('leaf', 'rows'))
The draws below stay inside these ranges and needn't reach their ends.
Inputs may be any that keep to these rules, and one draw needn't show every extreme that they name: `tree_order`: each aligned run of 1024 entries, the run starting at b * 1024, is a permutation of b * 1024 to (b + 1) * 1024 - 1. `mid_perm`: a permutation of 0 to 7.
All inputs are finite; a program needn't handle non-finite values.
Results may differ from the reference program's by a relative error of at most 0.025.
Values may be sent and summed in bfloat16 or wider, within the bound.
No kernel may reach another device: no remote copies, remote signals or barrier semaphores. Data moves between devices by JAX's collectives and lax.ppermute only.
A program may use at most 64 MiB of HBM per device.

```python
import math
import jax
import jax.numpy as jnp
from jax import lax

PTS = 1024
RANK = 48
RHS = 8
ITERS = 2
LEAVES = 8
ROWB = 4
NPTS = 32768
N_LEAF = 8
N_ROWS = 4


def draw_tree_order(key, part):
    blocks = NPTS // PTS
    upper_bound = (1 << 30) // PTS
    scores = jax.random.randint(jax.random.fold_in(key, 11), (blocks, PTS), 0, upper_bound, dtype=jnp.int32)
    scores = scores * PTS + jnp.arange(PTS, dtype=jnp.int32)[None, :]
    within = jnp.argsort(scores, axis=1).astype(jnp.int32)
    starts = (jnp.arange(blocks, dtype=jnp.int32) * PTS)[:, None]
    return (within + starts).reshape(NPTS).astype(jnp.int32)


def steps_of(own_key, dims, pieces, smallest, largest):
    gain, own = 1.0, jax.random.fold_in(own_key, 6)
    for dim, parts in pieces:
        draws = jnp.exp(jax.random.uniform(jax.random.fold_in(own, dim), (parts,), jnp.float32, smallest / len(pieces), largest / len(pieces)))
        gain = gain * jnp.repeat(draws, dims[dim] // parts).reshape([-1 if axis == dim else 1 for axis in range(len(dims))])
    return gain


def scatter_about(own_key, dims, scale, most, cuts=(), kind=jnp.bfloat16):
    gain = steps_of(own_key, dims, cuts, -0.22, 0.18) if cuts else 1.0
    result = jax.random.normal(own_key, dims, jnp.float32) * scale * gain
    return jnp.minimum(jnp.maximum(result, -most), most).astype(kind)


def setup_inputs(seed: int = 0) -> dict:
    seeds = jax.random.split(jax.random.key(seed), 9)
    right_side = scatter_about(seeds[0], (RHS, NPTS), 1.0, 6.0, ((1, 32),), jnp.float32)
    diagonal = jnp.clip(jnp.exp(math.log(4.0) - 2.0794415 * jax.random.uniform(seeds[1], (NPTS,), jnp.float32) ** steps_of(seeds[1], (NPTS,), ((0, 32),), -0.2, 0.2)), 0.5, 4.0)
    tree_order = draw_tree_order(jax.random.fold_in(seeds[8], 71), 0)
    mid_perm = jax.random.permutation(seeds[3], LEAVES).astype(jnp.int32)
    col_factor = scatter_about(seeds[4], (NPTS, LEAVES * RANK), PTS ** -0.5, 0.1875, ((0, 32),))
    mid_factor = scatter_about(seeds[5], (LEAVES * LEAVES * RANK, ROWB * ROWB * RANK), (LEAVES * ROWB * RANK) ** -0.5, 0.15625, ((0, 8), (1, 4)))
    pre_factor = scatter_about(seeds[6], (LEAVES * LEAVES * RANK, ROWB * ROWB * RANK), (LEAVES * ROWB * RANK) ** -0.5, 0.15625, ((0, 8), (1, 4)))
    row_factor = scatter_about(seeds[7], (RANK, NPTS), RANK ** -0.5, 0.875, ((1, 32),))
    return {"right_side": right_side, "diagonal": diagonal, "tree_order": tree_order, "mid_perm": mid_perm, "col_factor": col_factor, "mid_factor": mid_factor, "pre_factor": pre_factor, "row_factor": row_factor}


def gram_apply(field, tree_order, mid_perm, col_factor, mid_weight, row_factor):
    leaves = N_LEAF
    row_count = N_ROWS
    blocks = leaves * row_count
    sides = field.shape[0]
    taken = jnp.take(field, tree_order, axis=1).astype(jnp.bfloat16)
    taken = taken.reshape(sides, blocks, PTS).transpose(1, 0, 2)
    col_blocks = col_factor.reshape(blocks, PTS, leaves * RANK)

    def forward_map(inputs):
        block_field, block_factor = inputs
        return jnp.dot(block_field, block_factor, preferred_element_type=jnp.float32).astype(jnp.bfloat16)

    coeffs = lax.map(forward_map, (taken, col_blocks)).reshape(blocks, sides, leaves, RANK)
    outgoing = coeffs[:, :, mid_perm, :]
    outgoing = outgoing.reshape(leaves, row_count, sides, leaves, RANK).transpose(3, 0, 1, 2, 4)
    mid_blocks = mid_weight.reshape(leaves, leaves, RANK, row_count, row_count * RANK)

    def middle_map(inputs):
        group_coef, group_weight = inputs
        return jnp.einsum('lrsk,lkrm->sm', group_coef.astype(jnp.float32), group_weight.astype(jnp.float32),
                          precision=lax.Precision.HIGHEST)

    head_coef = lax.map(middle_map, (outgoing, mid_blocks))
    head_coef = head_coef.reshape(leaves, sides, row_count, RANK).transpose(0, 2, 1, 3)
    head_coef = head_coef.reshape(blocks, sides, RANK).astype(jnp.bfloat16)
    row_blocks = row_factor.astype(jnp.float32).reshape(RANK, blocks, PTS).transpose(1, 0, 2)
    image_tree = jnp.einsum('bsk,bkn->bsn', head_coef.astype(jnp.float32), row_blocks,
                            precision=lax.Precision.HIGHEST)
    backward = jnp.einsum('bsn,bkn->bsk', image_tree, row_blocks,
                          precision=lax.Precision.HIGHEST).astype(jnp.bfloat16)
    backward = backward.reshape(leaves, row_count, sides, RANK).transpose(0, 2, 1, 3)
    backward = backward.reshape(leaves, sides, row_count * RANK)

    def middle_back(inputs):
        group_back, group_weight = inputs
        return jnp.einsum('sm,lkrm->rlsk', group_back.astype(jnp.float32), group_weight.astype(jnp.float32),
                          precision=lax.Precision.HIGHEST).astype(jnp.bfloat16)

    returned = lax.map(middle_back, (backward, mid_blocks))
    returned = returned.transpose(2, 1, 0, 3, 4).reshape(blocks, leaves, sides, RANK)
    unsent = jnp.zeros_like(returned).at[:, mid_perm].set(returned)

    def backward_map(inputs):
        block_coef, block_factor = inputs
        flattened = block_coef.transpose(1, 0, 2).reshape(sides, leaves * RANK)
        return jnp.dot(flattened, block_factor.T, preferred_element_type=jnp.float32)

    gram_tree = lax.map(backward_map, (unsent, col_blocks))
    gram_tree = gram_tree.transpose(1, 0, 2).reshape(sides, blocks * PTS)
    return jnp.zeros_like(gram_tree).at[:, tree_order].set(gram_tree)


def reference(right_side, diagonal, tree_order, mid_perm, col_factor, mid_factor, pre_factor, row_factor):
    def apply_system(field):
        return diagonal[None, :] * field + gram_apply(field, tree_order, mid_perm, col_factor, mid_factor, row_factor)

    def apply_precond(field):
        return field / diagonal[None, :] + gram_apply(field, tree_order, mid_perm, col_factor, pre_factor, row_factor)

    solution = jnp.zeros_like(right_side)
    residual = right_side
    precond = apply_precond(residual)
    direction = precond
    precond_dot = jnp.sum(residual * precond, axis=1)
    for iteration in range(ITERS):
        image = apply_system(direction)
        alpha_step = precond_dot / jnp.sum(direction * image, axis=1)
        solution = solution + alpha_step[:, None] * direction
        residual = residual - alpha_step[:, None] * image
        if iteration + 1 < ITERS:
            precond = apply_precond(residual)
            dot_next = jnp.sum(residual * precond, axis=1)
            direction = precond + (dot_next / precond_dot)[:, None] * direction
            precond_dot = dot_next
    return solution, residual
```

```python
import jax
import jax.numpy as jnp
from jax import lax
from jax.sharding import PartitionSpec as P

ITERS = 2
LANES = 128


def widen(values, width):
    pads = [(0, 0)] * (values.ndim - 1) + [(0, width - values.shape[-1])]
    return jnp.pad(values, pads)


def per_device(
    right_side, diagonal, tree_order, mid_perm, col_factor, mid_factor, pre_factor, row_factor
):
    sides, points = right_side.shape
    rank_size = row_factor.shape[0]
    leaves = mid_perm.shape[0]
    row_count = mid_factor.shape[1] // rank_size
    width = -(-(rank_size + 1) // LANES) * LANES
    row = lax.axis_index("rows")
    shifts = jnp.arange(row_count, dtype=jnp.int32)
    sources = (row - shifts) % row_count

    def gather_rows(block):
        pieces = [block]
        for shift in range(1, row_count):
            ring = [(i, (i + shift) % row_count) for i in range(row_count)]
            pieces.append(lax.ppermute(block, "rows", ring))
        return [piece.reshape(leaves, rank_size, row_count * rank_size) for piece in pieces]

    own_gram = jnp.dot(row_factor, row_factor.T, preferred_element_type=jnp.float32)
    gram_blocks = lax.all_gather(own_gram[None], "rows", axis=0, tiled=True)
    pre_pieces = gather_rows(pre_factor)
    mid_pieces = gather_rows(mid_factor)

    local_index = tree_order % points
    point_ids = jnp.arange(points, dtype=jnp.int32)
    place = (point_ids[:, None] == local_index[None, :]).astype(jnp.bfloat16)
    slot_ids = jnp.arange(leaves, dtype=jnp.int32)
    onehot = (mid_perm[:, None] == slot_ids[None, :]).astype(jnp.bfloat16)
    columns = jnp.dot(place, col_factor, preferred_element_type=jnp.float32).astype(jnp.bfloat16)
    columns = columns.reshape(points, leaves, rank_size)
    columns = jnp.einsum(
        "qg,ngk->nqk", onehot, columns, preferred_element_type=jnp.float32
    ).astype(jnp.bfloat16)

    def gram_apply(field, pieces, local_dot):
        coeffs = jnp.einsum(
            "sn,nqk->qsk", field.astype(jnp.bfloat16), columns, preferred_element_type=jnp.float32
        )
        dots = jnp.broadcast_to(local_dot[None, :, None], (leaves, sides, 1))
        outgoing = widen(jnp.concatenate([coeffs, dots], axis=2), width)
        outgoing = jnp.broadcast_to(
            outgoing[:, None], (leaves, row_count, sides, width)
        ).reshape(leaves * row_count, sides, width)
        incoming = lax.all_to_all(
            outgoing, ("leaf", "rows"), split_axis=0, concat_axis=0, tiled=True
        )
        local_total = jnp.sum(incoming[:, :, rank_size], axis=0)
        incoming = incoming[:, :, :rank_size].astype(jnp.bfloat16)
        incoming = incoming.reshape(leaves, row_count, sides, rank_size)
        incoming = jnp.take(incoming, sources, axis=1)
        totals = 0.0
        for shift in range(row_count):
            totals = totals + jnp.einsum(
                "lsk,lkm->sm",
                incoming[:, shift],
                pieces[shift],
                preferred_element_type=jnp.float32,
            )
        head_coef = totals.astype(jnp.bfloat16).astype(jnp.float32)
        head_coef = head_coef.reshape(sides, row_count, rank_size)
        gathered = jnp.einsum(
            "sjk,jkm->sjm", head_coef, gram_blocks, precision=lax.Precision.HIGHEST
        )
        own_dot = jnp.sum(head_coef * gathered, axis=(1, 2))
        gathered = gathered.reshape(sides, row_count * rank_size).astype(jnp.bfloat16)
        returned = jnp.einsum(
            "sm,lkm->lsk", gathered, pieces[0], preferred_element_type=jnp.float32
        )
        dots = jnp.broadcast_to(own_dot[None, :, None], (leaves, sides, 1))
        returned = widen(jnp.concatenate([returned, dots], axis=2), width)
        arrived = lax.all_to_all(returned, "leaf", split_axis=0, concat_axis=0, tiled=True)
        total_dot = local_total + jnp.sum(arrived[:, :, rank_size], axis=0)
        unsent = arrived[:, :, :rank_size].astype(jnp.bfloat16)
        image = jnp.einsum("qsk,nqk->sn", unsent, columns, preferred_element_type=jnp.float32)
        return image, total_dot

    def apply_precond(field):
        scaled = field / diagonal[None, :]
        image, total = gram_apply(field, pre_pieces, jnp.sum(field * scaled, axis=1))
        return scaled + image, total

    def apply_system(field):
        scaled = field * diagonal[None, :]
        image, total = gram_apply(field, mid_pieces, jnp.sum(field * scaled, axis=1))
        return scaled + image, total

    solution = jnp.zeros_like(right_side)
    residual = right_side
    direction, residual_dot = apply_precond(residual)
    for iteration in range(ITERS):
        image, curvature = apply_system(direction)
        alpha_step = residual_dot / curvature
        solution = solution + alpha_step[:, None] * direction
        residual = residual - alpha_step[:, None] * image
        if iteration + 1 < ITERS:
            precond, dot_next = apply_precond(residual)
            direction = precond + (dot_next / residual_dot)[:, None] * direction
            residual_dot = dot_next
    return (solution, residual)


def solution(mesh):
    return jax.shard_map(
        per_device,
        mesh=mesh,
        in_specs=(
            P(None, ("leaf", "rows")),
            P(("leaf", "rows")),
            P(("leaf", "rows")),
            P(),
            P(("leaf", "rows"), None),
            P("leaf", "rows"),
            P("leaf", "rows"),
            P(None, ("leaf", "rows")),
        ),
        out_specs=(P(None, ("leaf", "rows")), P(None, ("leaf", "rows"))),
        check_vma=False,
    )
```

```python
import jax
import jax.numpy as jnp
from jax import lax
from jax.experimental import pallas as pl
from jax.experimental.pallas import tpu as pltpu
from jax.sharding import PartitionSpec as P

ITERS = 2
LANES = 128
F32 = jnp.float32
BF16 = jnp.bfloat16
VMEM = pl.BlockSpec(memory_space=pltpu.VMEM)
SMEM = pl.BlockSpec(memory_space=pltpu.SMEM)
TRANSPOSED = (((1,), (1,)), ((), ()))


def call(body, args, out_shape, scalars=0):
    specs = [SMEM] * scalars + [VMEM] * (len(args) - scalars)
    return pl.pallas_call(
        body,
        in_specs=specs,
        out_specs=jax.tree.map(lambda _: VMEM, out_shape),
        out_shape=out_shape,
    )(*args)


def dot_lanes(value, spare):
    high = value.astype(BF16).astype(F32)
    middle = (value - high).astype(BF16).astype(F32)
    low = value - high - middle
    lane = lax.broadcasted_iota(jnp.int32, (value.shape[0], spare), 1)
    parts = jnp.where(lane == 0, high, jnp.where(lane == 1, middle, 0.0))
    return jnp.where(lane == 2, low, parts)


def pack(values, index, rank_size, extras):
    piece = values[:, index * rank_size : (index + 1) * rank_size]
    return jnp.concatenate([piece, extras], axis=1).astype(BF16)


def unpack(blocks, rank_size):
    wide = [block.astype(F32) for block in blocks]
    carried = wide[0]
    for block in wide[1:]:
        carried = carried + block
    joined = jnp.concatenate([block[:, :rank_size] for block in wide], axis=1).astype(BF16)
    lane = lax.broadcasted_iota(jnp.int32, carried.shape, 1)
    carried = jnp.where((lane >= rank_size) & (lane < rank_size + 3), carried, 0.0)
    return joined, jnp.sum(carried, axis=1, keepdims=True)


def middle_stage(sources, incoming, gram_high, gram_low, pieces, rank_size):
    leaves, row_count, sides, width = incoming.shape

    def body(sources_ref, incoming_ref, high_ref, low_ref, *refs):
        piece_refs = refs[:row_count]
        out_ref, total_ref = refs[row_count:]
        totals = 0.0
        carried = 0.0
        for shift in range(row_count):
            source = sources_ref[shift]
            blocks = [incoming_ref[leaf, source] for leaf in range(leaves)]
            joined, dots = unpack(blocks, rank_size)
            carried = carried + dots
            totals = totals + jnp.dot(
                joined, piece_refs[shift][...], preferred_element_type=F32
            )
        head_coef = totals.astype(BF16)
        gathered = jnp.dot(head_coef, high_ref[...], preferred_element_type=F32)
        gathered = gathered + jnp.dot(head_coef, low_ref[...], preferred_element_type=F32)
        returned = lax.dot_general(
            gathered.astype(BF16), piece_refs[0][...], TRANSPOSED, preferred_element_type=F32
        )
        own_dot = jnp.sum(head_coef.astype(F32) * gathered, axis=1, keepdims=True)
        extras = dot_lanes(own_dot, width - rank_size)
        for leaf in range(leaves):
            out_ref[leaf] = pack(returned, leaf, rank_size, extras)
        total_ref[...] = jnp.broadcast_to(carried, (sides, LANES))

    return call(
        body,
        (sources, incoming, gram_high, gram_low, *pieces),
        (
            jax.ShapeDtypeStruct((leaves, sides, width), BF16),
            jax.ShapeDtypeStruct((sides, LANES), F32),
        ),
        scalars=1,
    )


def block_stage(update, state, columns, diagonal, arrived, local_total, sizes, send, keep):
    leaves, row_count, sides, points, rank_size, width = sizes
    returns = arrived is not None
    kept = [
        jax.ShapeDtypeStruct((sides, points if full else LANES), F32) for full in keep
    ]
    sent = [jax.ShapeDtypeStruct((leaves, row_count, sides, width), BF16)] if send else []
    args = [columns, diagonal[None, :]] + ([arrived, local_total] if returns else [])
    first = len(args)
    args += state

    def body(*refs):
        outs = refs[len(args) :]
        columns_ref, diagonal_ref = refs[:2]
        image = total = None
        if returns:
            joined, dots = unpack([refs[2][leaf] for leaf in range(leaves)], rank_size)
            total = refs[3][:, :1] + dots
            image = lax.dot_general(
                joined, columns_ref[...], TRANSPOSED, preferred_element_type=F32
            )
        values = [ref[...] for ref in refs[first : len(args)]]
        results, field, scaled = update(image, total, diagonal_ref[...], *values)
        for ref, value in zip(outs, results):
            ref[...] = jnp.broadcast_to(value, ref.shape)
        if send:
            coeffs = jnp.dot(field.astype(BF16), columns_ref[...], preferred_element_type=F32)
            own_dot = jnp.sum(field * scaled, axis=1, keepdims=True)
            extras = dot_lanes(own_dot, width - rank_size)
            for leaf in range(leaves):
                chunk = pack(coeffs, leaf, rank_size, extras)
                for row in range(row_count):
                    outs[len(kept)][leaf, row] = chunk

    return call(body, args, tuple(kept + sent))


def start_step(image, total, diagonal, right_side):
    return (), right_side, right_side / diagonal


def first_direction(image, total, diagonal, residual):
    direction = residual / diagonal + image
    return (direction, total), direction, direction * diagonal


def advance(image, total, diagonal, direction, residual, solution, residual_dot):
    image = direction * diagonal + image
    alpha_step = residual_dot[:, :1] / total
    solution = solution + alpha_step * direction
    residual = residual - alpha_step * image
    return (solution, residual), residual, residual / diagonal


def next_direction(image, total, diagonal, direction, residual, residual_dot):
    precond = residual / diagonal + image
    direction = precond + (total / residual_dot[:, :1]) * direction
    return (direction, total), direction, direction * diagonal


def per_device(
    right_side, diagonal, tree_order, mid_perm, col_factor, mid_factor, pre_factor, row_factor
):
    sides, points = right_side.shape
    rank_size = row_factor.shape[0]
    leaves = mid_perm.shape[0]
    row_count = mid_factor.shape[1] // rank_size
    width = -(-(rank_size + 3) // LANES) * LANES
    row = lax.axis_index("rows")
    shifts = jnp.arange(row_count, dtype=jnp.int32)
    sources = (row - shifts) % row_count

    def gather_rows(block):
        pieces = [block]
        for shift in range(1, row_count):
            ring = [(i, (i + shift) % row_count) for i in range(row_count)]
            pieces.append(lax.ppermute(block, "rows", ring))
        return pieces

    own_gram = jnp.dot(row_factor, row_factor.T, preferred_element_type=F32)
    gram_pieces = jnp.stack(gather_rows(own_gram))
    pre_pieces = gather_rows(pre_factor)
    mid_pieces = gather_rows(mid_factor)
    grams = jnp.take(gram_pieces, (row - shifts) % row_count, axis=0)
    same = (shifts[:, None] == shifts[None, :]).astype(F32)
    gram = grams[:, :, None, :] * same[:, None, :, None]
    gram = gram.reshape(row_count * rank_size, row_count * rank_size)
    gram_high = lax.reduce_precision(gram, 8, 7)
    gram_low = (gram - gram_high).astype(BF16)
    gram_high = gram_high.astype(BF16)

    local_index = tree_order % points
    point_ids = jnp.arange(points, dtype=jnp.int32)
    place = (point_ids[:, None] == local_index[None, :]).astype(BF16)
    columns = jnp.dot(place, col_factor, preferred_element_type=F32).astype(BF16)
    slots = (mid_perm[:, None] * rank_size + jnp.arange(rank_size)[None, :]).reshape(-1)
    column_ids = jnp.arange(leaves * rank_size, dtype=jnp.int32)
    move = (column_ids[:, None] == slots[None, :]).astype(BF16)
    columns = jnp.dot(columns, move, preferred_element_type=F32).astype(BF16)
    sizes = (leaves, row_count, sides, points, rank_size, width)

    def exchange(outgoing, pieces):
        incoming = lax.all_to_all(
            outgoing.reshape(leaves * row_count, sides, width),
            ("leaf", "rows"),
            split_axis=0,
            concat_axis=0,
            tiled=True,
        )
        incoming = incoming.reshape(leaves, row_count, sides, width)
        returned, local_total = middle_stage(
            sources, incoming, gram_high, gram_low, pieces, rank_size
        )
        arrived = lax.all_to_all(returned, "leaf", split_axis=0, concat_axis=0, tiled=True)
        return arrived, local_total

    def stage(update, state, received, send, keep):
        return block_stage(update, state, columns, diagonal, *received, sizes, send, keep)

    (outgoing,) = stage(start_step, [right_side], (None, None), True, ())
    received = exchange(outgoing, pre_pieces)
    direction, residual_dot, outgoing = stage(
        first_direction, [right_side], received, True, (True, False)
    )
    solution = jnp.zeros_like(right_side)
    residual = right_side
    for iteration in range(ITERS):
        received = exchange(outgoing, mid_pieces)
        more = iteration + 1 < ITERS
        state = [direction, residual, solution, residual_dot]
        solution, residual, *sent = stage(advance, state, received, more, (True, True))
        if more:
            received = exchange(sent[0], pre_pieces)
            state = [direction, residual, residual_dot]
            direction, residual_dot, outgoing = stage(
                next_direction, state, received, True, (True, False)
            )
    return (solution, residual)


def solution(mesh):
    return jax.shard_map(
        per_device,
        mesh=mesh,
        in_specs=(
            P(None, ("leaf", "rows")),
            P(("leaf", "rows")),
            P(("leaf", "rows")),
            P(),
            P(("leaf", "rows"), None),
            P("leaf", "rows"),
            P("leaf", "rows"),
            P(None, ("leaf", "rows")),
        ),
        out_specs=(P(None, ("leaf", "rows")), P(None, ("leaf", "rows"))),
        check_vma=False,
    )
```

```python
import jax
import jax.numpy as jnp
from jax import lax
from jax.experimental import pallas as pl
from jax.experimental.pallas import tpu as pltpu
from jax.sharding import PartitionSpec as P

ITERS = 2
LANES = 128
NEAR_BYTES = 1 << 20
F32 = jnp.float32
BF16 = jnp.bfloat16
VMEM = pl.BlockSpec(memory_space=pltpu.VMEM)
SMEM = pl.BlockSpec(memory_space=pltpu.SMEM)
TRANSPOSED = (((1,), (1,)), ((), ()))


def call(body, args, out_shape, scalars=0):
    specs = [SMEM] * scalars + [VMEM] * (len(args) - scalars)
    args = [
        pltpu.with_memory_space_constraint(arg, pltpu.VMEM)
        if at >= scalars and arg.size * arg.dtype.itemsize <= NEAR_BYTES
        else arg
        for at, arg in enumerate(args)
    ]
    return pl.pallas_call(
        body,
        in_specs=specs,
        out_specs=jax.tree.map(lambda _: VMEM, out_shape),
        out_shape=out_shape,
    )(*args)


def dot_lanes(value, spare):
    high = value.astype(BF16).astype(F32)
    middle = (value - high).astype(BF16).astype(F32)
    low = value - high - middle
    lane = lax.broadcasted_iota(jnp.int32, (value.shape[0], spare), 1)
    parts = jnp.where(lane == 0, high, jnp.where(lane == 1, middle, 0.0))
    return jnp.where(lane == 2, low, parts)


def pack(values, index, rank_size, extras):
    piece = values[:, index * rank_size : (index + 1) * rank_size]
    return jnp.concatenate([piece, extras], axis=1).astype(BF16)


def unpack(blocks, rank_size):
    wide = [block.astype(F32) for block in blocks]
    carried = wide[0]
    for block in wide[1:]:
        carried = carried + block
    joined = jnp.concatenate([block[:, :rank_size] for block in wide], axis=1).astype(BF16)
    lane = lax.broadcasted_iota(jnp.int32, carried.shape, 1)
    carried = jnp.where((lane >= rank_size) & (lane < rank_size + 3), carried, 0.0)
    return joined, jnp.sum(carried, axis=1, keepdims=True)


def middle_stage(sources, incoming, gram_high, gram_low, pieces, rank_size):
    leaves, row_count, sides, width = incoming.shape

    def body(sources_ref, incoming_ref, high_ref, low_ref, *refs):
        piece_refs = refs[:row_count]
        out_ref, total_ref = refs[row_count:]
        totals = 0.0
        carried = 0.0
        for shift in range(row_count):
            source = sources_ref[shift]
            blocks = [incoming_ref[leaf, source] for leaf in range(leaves)]
            joined, dots = unpack(blocks, rank_size)
            carried = carried + dots
            totals = totals + jnp.dot(
                joined, piece_refs[shift][...], preferred_element_type=F32
            )
        head_coef = totals.astype(BF16)
        gathered = jnp.dot(head_coef, high_ref[...], preferred_element_type=F32)
        gathered = gathered + jnp.dot(head_coef, low_ref[...], preferred_element_type=F32)
        returned = lax.dot_general(
            gathered.astype(BF16), piece_refs[0][...], TRANSPOSED, preferred_element_type=F32
        )
        own_dot = jnp.sum(head_coef.astype(F32) * gathered, axis=1, keepdims=True)
        extras = dot_lanes(own_dot, width - rank_size)
        for leaf in range(leaves):
            out_ref[leaf] = pack(returned, leaf, rank_size, extras)
        total_ref[...] = jnp.broadcast_to(carried, (sides, LANES))

    return call(
        body,
        (sources, incoming, gram_high, gram_low, *pieces),
        (
            pltpu.VMEM((leaves, sides, width), BF16),
            pltpu.VMEM((sides, LANES), F32),
        ),
        scalars=1,
    )


def block_stage(update, state, columns, diagonal, arrived, local_total, sizes, send, keep):
    leaves, row_count, sides, points, rank_size, width = sizes
    returns = arrived is not None
    kind = pltpu.VMEM if send else jax.ShapeDtypeStruct
    kept = [kind((sides, points if full else LANES), F32) for full in keep]
    sent = [kind((leaves, row_count, sides, width), BF16)] if send else []
    args = [columns, diagonal[None, :]] + ([arrived, local_total] if returns else [])
    first = len(args)
    args += state

    def body(*refs):
        outs = refs[len(args) :]
        columns_ref, diagonal_ref = refs[:2]
        image = total = None
        if returns:
            joined, dots = unpack([refs[2][leaf] for leaf in range(leaves)], rank_size)
            total = refs[3][:, :1] + dots
            image = lax.dot_general(
                joined, columns_ref[...], TRANSPOSED, preferred_element_type=F32
            )
        values = [ref[...] for ref in refs[first : len(args)]]
        results, field, scaled = update(image, total, diagonal_ref[...], *values)
        for ref, value in zip(outs, results):
            ref[...] = jnp.broadcast_to(value, ref.shape)
        if send:
            coeffs = jnp.dot(field.astype(BF16), columns_ref[...], preferred_element_type=F32)
            own_dot = jnp.sum(field * scaled, axis=1, keepdims=True)
            extras = dot_lanes(own_dot, width - rank_size)
            for leaf in range(leaves):
                chunk = pack(coeffs, leaf, rank_size, extras)
                for row in range(row_count):
                    outs[len(kept)][leaf, row] = chunk

    return call(body, args, tuple(kept + sent))


def start_step(image, total, diagonal, right_side):
    return (), right_side, right_side / diagonal


def first_direction(image, total, diagonal, residual):
    direction = residual / diagonal + image
    return (direction, total), direction, direction * diagonal


def advance(image, total, diagonal, residual_dot, direction, residual, *solution):
    image = direction * diagonal + image
    alpha_step = residual_dot[:, :1] / total
    solution = sum(solution, alpha_step * direction)
    residual = residual - alpha_step * image
    return (solution, residual), residual, residual / diagonal


def next_direction(image, total, diagonal, direction, residual, residual_dot):
    precond = residual / diagonal + image
    direction = precond + (total / residual_dot[:, :1]) * direction
    return (direction, total), direction, direction * diagonal


def per_device(
    right_side, diagonal, tree_order, mid_perm, col_factor, mid_factor, pre_factor, row_factor
):
    sides, points = right_side.shape
    rank_size = row_factor.shape[0]
    leaves = mid_perm.shape[0]
    row_count = mid_factor.shape[1] // rank_size
    width = -(-(rank_size + 3) // LANES) * LANES
    row = lax.axis_index("rows")
    shifts = jnp.arange(row_count, dtype=jnp.int32)
    sources = (row - shifts) % row_count

    def gather_rows(block):
        pieces = [block]
        for shift in range(1, row_count):
            ring = [(i, (i + shift) % row_count) for i in range(row_count)]
            pieces.append(lax.ppermute(block, "rows", ring))
        return pieces

    own_gram = jnp.dot(row_factor, row_factor.T, preferred_element_type=F32)
    grams = lax.all_gather(own_gram[None], "rows", axis=0, tiled=True)
    pre_pieces = gather_rows(pre_factor)
    mid_pieces = gather_rows(mid_factor)
    same = (shifts[:, None] == shifts[None, :]).astype(F32)
    gram = grams[:, :, None, :] * same[:, None, :, None]
    gram = gram.reshape(row_count * rank_size, row_count * rank_size)
    gram_high = lax.reduce_precision(gram, 8, 7)
    gram_low = (gram - gram_high).astype(BF16)
    gram_high = gram_high.astype(BF16)

    local_index = tree_order % points
    point_ids = jnp.arange(points, dtype=jnp.int32)
    place = (point_ids[:, None] == local_index[None, :]).astype(BF16)
    columns = jnp.dot(place, col_factor, preferred_element_type=F32).astype(BF16)
    slot_ids = jnp.arange(leaves, dtype=jnp.int32)
    onehot = (mid_perm[:, None] == slot_ids[None, :]).astype(BF16)
    columns = jnp.einsum(
        "qg,ngk->nqk",
        onehot,
        columns.reshape(points, leaves, rank_size),
        preferred_element_type=F32,
    ).astype(BF16)
    columns = columns.reshape(points, leaves * rank_size)
    sizes = (leaves, row_count, sides, points, rank_size, width)

    def exchange(outgoing, pieces):
        incoming = lax.all_to_all(
            outgoing.reshape(leaves * row_count, sides, width),
            ("leaf", "rows"),
            split_axis=0,
            concat_axis=0,
            tiled=True,
        )
        incoming = incoming.reshape(leaves, row_count, sides, width)
        returned, local_total = middle_stage(
            sources, incoming, gram_high, gram_low, pieces, rank_size
        )
        arrived = lax.all_to_all(returned, "leaf", split_axis=0, concat_axis=0, tiled=True)
        return arrived, local_total

    def stage(update, state, received, send, keep):
        return block_stage(update, state, columns, diagonal, *received, sizes, send, keep)

    (outgoing,) = stage(start_step, [right_side], (None, None), True, ())
    received = exchange(outgoing, pre_pieces)
    direction, residual_dot, outgoing = stage(
        first_direction, [right_side], received, True, (True, False)
    )
    solution = []
    residual = right_side
    for iteration in range(ITERS):
        received = exchange(outgoing, mid_pieces)
        more = iteration + 1 < ITERS
        state = [residual_dot, direction, residual] + solution
        outs = stage(advance, state, received, more, (True, True))
        solution, residual, sent = [outs[0]], outs[1], outs[2:]
        if more:
            received = exchange(sent[0], pre_pieces)
            state = [direction, residual, residual_dot]
            direction, residual_dot, outgoing = stage(
                next_direction, state, received, True, (True, False)
            )
    return (solution[0], residual)


def solution(mesh):
    return jax.shard_map(
        per_device,
        mesh=mesh,
        in_specs=(
            P(None, ("leaf", "rows")),
            P(("leaf", "rows")),
            P(("leaf", "rows")),
            P(),
            P(("leaf", "rows"), None),
            P("leaf", "rows"),
            P("leaf", "rows"),
            P(None, ("leaf", "rows")),
        ),
        out_specs=(P(None, ("leaf", "rows")), P(None, ("leaf", "rows"))),
        check_vma=False,
    )
```

```python
import jax
import jax.numpy as jnp
from jax import lax
from jax.experimental import pallas as pl
from jax.experimental.pallas import tpu as pltpu
from jax.sharding import PartitionSpec as P

ITERS = 2
LANES = 128
NEAR_BYTES = 1 << 20
F32 = jnp.float32
BF16 = jnp.bfloat16
VMEM = pl.BlockSpec(memory_space=pltpu.VMEM)
SMEM = pl.BlockSpec(memory_space=pltpu.SMEM)
TRANSPOSED = (((1,), (1,)), ((), ()))


def call(body, args, out_shape, scalars=0):
    specs = [SMEM] * scalars + [VMEM] * (len(args) - scalars)
    args = [
        pltpu.with_memory_space_constraint(arg, pltpu.VMEM)
        if at >= scalars and arg.size * arg.dtype.itemsize <= NEAR_BYTES
        else arg
        for at, arg in enumerate(args)
    ]
    return pl.pallas_call(
        body,
        in_specs=specs,
        out_specs=jax.tree.map(lambda _: VMEM, out_shape),
        out_shape=out_shape,
    )(*args)


def dot_lanes(value, spare):
    high = value.astype(BF16).astype(F32)
    middle = (value - high).astype(BF16).astype(F32)
    low = value - high - middle
    lane = lax.broadcasted_iota(jnp.int32, (value.shape[0], spare), 1)
    parts = jnp.where(lane == 0, high, jnp.where(lane == 1, middle, 0.0))
    return jnp.where(lane == 2, low, parts)


def pack(values, index, rank_size, extras):
    piece = values[:, index * rank_size : (index + 1) * rank_size]
    return jnp.concatenate([piece, extras], axis=1).astype(BF16)


def unpack(blocks, rank_size):
    wide = [block.astype(F32) for block in blocks]
    carried = wide[0]
    for block in wide[1:]:
        carried = carried + block
    joined = jnp.concatenate([block[:, :rank_size] for block in wide], axis=1).astype(BF16)
    lane = lax.broadcasted_iota(jnp.int32, carried.shape, 1)
    carried = jnp.where((lane >= rank_size) & (lane < rank_size + 3), carried, 0.0)
    return joined, jnp.sum(carried, axis=1, keepdims=True)


def place_columns(local_index, slots, col_factor):
    def body(index_ref, slots_ref, factor_ref, out_ref):
        points, wide = out_ref.shape
        ids = lax.broadcasted_iota(jnp.int32, (points, points), 0)
        place = (ids == index_ref[...]).astype(F32).astype(BF16)
        placed = jnp.dot(place, factor_ref[...], preferred_element_type=F32).astype(BF16)
        ids = lax.broadcasted_iota(jnp.int32, (wide, wide), 0)
        move = (ids == slots_ref[...]).astype(F32).astype(BF16)
        out_ref[...] = jnp.dot(placed, move, preferred_element_type=F32).astype(BF16)

    near = col_factor.size * col_factor.dtype.itemsize <= NEAR_BYTES
    kind = pltpu.VMEM if near else jax.ShapeDtypeStruct
    args = (local_index[None, :], slots[None, :], col_factor)
    return call(body, args, kind(col_factor.shape, BF16))


def middle_stage(sources, incoming, gram_high, gram_low, pieces, rank_size):
    leaves, row_count, sides, width = incoming.shape

    def body(sources_ref, incoming_ref, high_ref, low_ref, *refs):
        piece_refs = refs[:row_count]
        out_ref, total_ref = refs[row_count:]
        totals = 0.0
        carried = 0.0
        for shift in range(row_count):
            source = sources_ref[shift]
            blocks = [incoming_ref[leaf, source] for leaf in range(leaves)]
            joined, dots = unpack(blocks, rank_size)
            carried = carried + dots
            totals = totals + jnp.dot(
                joined, piece_refs[shift][...], preferred_element_type=F32
            )
        head_coef = totals.astype(BF16)
        gathered = jnp.dot(head_coef, high_ref[...], preferred_element_type=F32)
        gathered = gathered + jnp.dot(head_coef, low_ref[...], preferred_element_type=F32)
        returned = lax.dot_general(
            gathered.astype(BF16), piece_refs[0][...], TRANSPOSED, preferred_element_type=F32
        )
        own_dot = jnp.sum(head_coef.astype(F32) * gathered, axis=1, keepdims=True)
        extras = dot_lanes(own_dot, width - rank_size)
        for leaf in range(leaves):
            out_ref[leaf] = pack(returned, leaf, rank_size, extras)
        total_ref[...] = jnp.broadcast_to(carried, (sides, LANES))

    return call(
        body,
        (sources, incoming, gram_high, gram_low, *pieces),
        (
            pltpu.VMEM((leaves, sides, width), BF16),
            pltpu.VMEM((sides, LANES), F32),
        ),
        scalars=1,
    )


def block_stage(update, state, columns, diagonal, arrived, local_total, sizes, send, keep):
    leaves, row_count, sides, points, rank_size, width = sizes
    returns = arrived is not None
    kind = pltpu.VMEM if send else jax.ShapeDtypeStruct
    kept = [kind((sides, points if full else LANES), F32) for full in keep]
    sent = [kind((leaves, row_count, sides, width), BF16)] if send else []
    args = [columns, diagonal[None, :]] + ([arrived, local_total] if returns else [])
    first = len(args)
    args += state

    def body(*refs):
        outs = refs[len(args) :]
        columns_ref, diagonal_ref = refs[:2]
        image = total = None
        if returns:
            joined, dots = unpack([refs[2][leaf] for leaf in range(leaves)], rank_size)
            total = refs[3][:, :1] + dots
            image = lax.dot_general(
                joined, columns_ref[...], TRANSPOSED, preferred_element_type=F32
            )
        values = [ref[...] for ref in refs[first : len(args)]]
        results, field, scaled = update(image, total, diagonal_ref[...], *values)
        for ref, value in zip(outs, results):
            ref[...] = jnp.broadcast_to(value, ref.shape)
        if send:
            coeffs = jnp.dot(field.astype(BF16), columns_ref[...], preferred_element_type=F32)
            own_dot = jnp.sum(field * scaled, axis=1, keepdims=True)
            extras = dot_lanes(own_dot, width - rank_size)
            for leaf in range(leaves):
                chunk = pack(coeffs, leaf, rank_size, extras)
                for row in range(row_count):
                    outs[len(kept)][leaf, row] = chunk

    return call(body, args, tuple(kept + sent))


def start_step(image, total, diagonal, right_side):
    return (), right_side, right_side / diagonal


def first_direction(image, total, diagonal, residual):
    direction = residual / diagonal + image
    return (direction, total), direction, direction * diagonal


def advance(image, total, diagonal, residual_dot, direction, residual, *solution):
    image = direction * diagonal + image
    alpha_step = residual_dot[:, :1] / total
    solution = sum(solution, alpha_step * direction)
    residual = residual - alpha_step * image
    return (solution, residual), residual, residual / diagonal


def next_direction(image, total, diagonal, direction, residual, residual_dot):
    precond = residual / diagonal + image
    direction = precond + (total / residual_dot[:, :1]) * direction
    return (direction, total), direction, direction * diagonal


def per_device(
    right_side, diagonal, tree_order, mid_perm, col_factor, mid_factor, pre_factor, row_factor
):
    sides, points = right_side.shape
    rank_size = row_factor.shape[0]
    leaves = mid_perm.shape[0]
    row_count = mid_factor.shape[1] // rank_size
    width = -(-(rank_size + 3) // LANES) * LANES
    row = lax.axis_index("rows")
    shifts = jnp.arange(row_count, dtype=jnp.int32)
    sources = (row - shifts) % row_count

    def gather_rows(block):
        pieces = [block]
        for shift in range(1, row_count):
            ring = [(i, (i + shift) % row_count) for i in range(row_count)]
            pieces.append(lax.ppermute(block, "rows", ring))
        return pieces

    local_index = tree_order % points
    slots = (mid_perm[:, None] * rank_size + jnp.arange(rank_size)[None, :]).reshape(-1)
    columns = place_columns(local_index, slots, col_factor)
    sizes = (leaves, row_count, sides, points, rank_size, width)

    def exchange(outgoing, pieces):
        incoming = lax.all_to_all(
            outgoing.reshape(leaves * row_count, sides, width),
            ("leaf", "rows"),
            split_axis=0,
            concat_axis=0,
            tiled=True,
        )
        incoming = incoming.reshape(leaves, row_count, sides, width)
        returned, local_total = middle_stage(
            sources, incoming, gram_high, gram_low, pieces, rank_size
        )
        arrived = lax.all_to_all(returned, "leaf", split_axis=0, concat_axis=0, tiled=True)
        return arrived, local_total

    def stage(update, state, received, send, keep):
        return block_stage(update, state, columns, diagonal, *received, sizes, send, keep)

    (outgoing,) = stage(start_step, [right_side], (None, None), True, ())
    row_factor, pre_factor, outgoing = lax.optimization_barrier(
        (row_factor, pre_factor, outgoing)
    )
    own_gram = jnp.dot(row_factor, row_factor.T, preferred_element_type=F32)
    pre_pieces = gather_rows(pre_factor)
    grams = jnp.take(jnp.stack(gather_rows(own_gram)), sources, axis=0)
    same = (shifts[:, None] == shifts[None, :]).astype(F32)
    gram = grams[:, :, None, :] * same[:, None, :, None]
    gram = gram.reshape(row_count * rank_size, row_count * rank_size)
    gram_high = lax.reduce_precision(gram, 8, 7)
    gram_low = (gram - gram_high).astype(BF16)
    gram_high = gram_high.astype(BF16)
    received = exchange(outgoing, pre_pieces)
    mid_pieces = gather_rows(mid_factor)
    direction, residual_dot, outgoing = stage(
        first_direction, [right_side], received, True, (True, False)
    )
    solution = []
    residual = right_side
    for iteration in range(ITERS):
        received = exchange(outgoing, mid_pieces)
        more = iteration + 1 < ITERS
        state = [residual_dot, direction, residual] + solution
        outs = stage(advance, state, received, more, (True, True))
        solution, residual, sent = [outs[0]], outs[1], outs[2:]
        if more:
            received = exchange(sent[0], pre_pieces)
            state = [direction, residual, residual_dot]
            direction, residual_dot, outgoing = stage(
                next_direction, state, received, True, (True, False)
            )
    return (solution[0], residual)


def solution(mesh):
    return jax.shard_map(
        per_device,
        mesh=mesh,
        in_specs=(
            P(None, ("leaf", "rows")),
            P(("leaf", "rows")),
            P(("leaf", "rows")),
            P(),
            P(("leaf", "rows"), None),
            P("leaf", "rows"),
            P("leaf", "rows"),
            P(None, ("leaf", "rows")),
        ),
        out_specs=(P(None, ("leaf", "rows")), P(None, ("leaf", "rows"))),
        check_vma=False,
    )
```
